32 devices in a mesh: row: 8 (over y, x, core), col: 4 (over z).
Axes of the slice: x: 2, y: 2, z: 4, core: 2. Of those that a mesh axis runs over, the one named last changes fastest.
Arguments:
- tokens: bfloat16 [6144, 2048], P('row', 'col'), may hold values from -6 to 6
- out_grad: bfloat16 [6144, 2048], P('row', 'col'), may hold values from -768 to 768
- counts: int32 [8], P('row'), may hold values from 65 to 768
- block_moves: int32 [4, 3], replicated, may hold values from 0 to 7, as said below
- segment_ids: int32 [6144], P('row'), may hold values from 0 to 191, never falling along the last dimension, each value on 1 to 128 neighbouring positions
- gate_weight: bfloat16 [2048, 8192], P('row', 'col'), may hold values from -0.125 to 0.125
- up_weight: bfloat16 [2048, 8192], P('row', 'col'), may hold values from -0.125 to 0.125
- down_weight: bfloat16 [2048, 8192], P('row', 'col'), may hold values from -0.0625 to 0.0625
Outputs:
- hidden: bfloat16 [4096, 8192], P('row', 'col')
- gate_grad: float32 [2048, 8192], P('row', 'col')
- up_grad: float32 [2048, 8192], P('row', 'col')
- down_grad: float32 [2048, 8192], P('row', 'col')
The draws below stay inside these ranges and needn't reach their ends.
Inputs may be any that keep to these rules, and one draw needn't show every extreme that they name: `block_moves`: each row is (source rank, destination rank, block index); the block is a valid block of its source; no two rows share both source and destination, nor both source and block; a rank is the source of at most two rows or the destination of at most one, never both; after the moves every rank holds at most 4 valid blocks and some hold exactly 4. `segment_ids`: never falling along the whole array; each document covers 1 to 128 consecutive slots.
All inputs are finite; a program needn't handle non-finite values.
Results may differ from the reference program's by a relative error of at most 0.015.
Values may be sent and summed in bfloat16 or wider, within the bound.
A program may use at most 128 MiB of HBM per device.

```python
import math
import jax
import jax.numpy as jnp
import numpy as np
from jax import lax

D = 2048
F = 8192
BLOCK = 128
WORK = 4
CAP = 6
TOK_DEV = 768
TOKENS = 6144
MOVES = 4
N_ROW = 8


def rebalance_plan(key):
    perm_key, light_key, part_key, pick_key, flip_key = jax.random.split(key, 5)
    groups = N_ROW // 4
    half = N_ROW // 2
    pair_order = jax.random.permutation(perm_key, half).astype(jnp.int32).reshape(groups, 2)
    flips = jax.random.randint(flip_key, (groups, 2), 0, 2, dtype=jnp.int32)
    low_rank = pair_order
    high_rank = pair_order + half
    first_rank = jnp.where(flips == 0, low_rank, high_rank)
    second_rank = jnp.where(flips == 0, high_rank, low_rank)
    order_ranks = jnp.stack([first_rank[:, 0], second_rank[:, 0], first_rank[:, 1], second_rank[:, 1]], axis=1).astype(jnp.int32)
    spare_load = jax.random.randint(light_key, (groups,), 1, WORK + 1, dtype=jnp.int32)
    heavy_load = jnp.full((groups,), WORK + 2, jnp.int32)
    lean_load = jnp.full((groups,), WORK - 1, jnp.int32)
    all_loads = jnp.stack([heavy_load, lean_load, lean_load, spare_load], axis=1).reshape(-1)
    block_counts = jnp.zeros((N_ROW,), jnp.int32).at[order_ranks.reshape(-1)].set(all_loads)
    tail_fill = jax.random.randint(part_key, (N_ROW,), BLOCK // 2 + 1, BLOCK + 1, dtype=jnp.int32)
    counts = ((block_counts - 1) * BLOCK + tail_fill).astype(jnp.int32)
    chosen = jax.vmap(lambda sub_key: jax.random.permutation(sub_key, WORK + 2)[:2])(jax.random.split(pick_key, groups)).astype(jnp.int32)
    first_move = jnp.stack([order_ranks[:, 0], order_ranks[:, 1], chosen[:, 0]], axis=1)
    second_move = jnp.stack([order_ranks[:, 0], order_ranks[:, 2], chosen[:, 1]], axis=1)
    block_moves = jnp.stack([first_move, second_move], axis=1).reshape(N_ROW // 2, 3).astype(jnp.int32)
    return (counts, block_moves)


def draw_counts(key, part):
    return rebalance_plan(jax.random.fold_in(key, 11))[0]


def draw_block_moves(key, part):
    return rebalance_plan(jax.random.fold_in(key, 11))[1]


def level_of(key, extent, cuts, smallest, largest):
    loudness, own = 1.0, jax.random.fold_in(key, 6)
    for dim, shards_of in cuts:
        steps = jnp.exp(jax.random.uniform(jax.random.fold_in(own, dim), (shards_of,), jnp.float32, smallest / len(cuts), largest / len(cuts)))
        loudness = loudness * jnp.repeat(steps, extent[dim] // shards_of).reshape([-1 if axis == dim else 1 for axis in range(len(extent))])
    return loudness


def length_profile(number_of, total, reach, slope):
    loads = [(1 << 20) // math.isqrt(rank ** slope) + 1 for rank in range(2, number_of + 1)]
    surplus, given = total - reach - (number_of - 1), [1] * (number_of - 1)
    while surplus > 0:
        candidates = [i for i in range(number_of - 1) if given[i] < reach]
        mass, left = sum([loads[i] for i in candidates]), surplus
        for i in candidates:
            extra = min(reach - given[i], max(1, left * loads[i] // mass), surplus)
            given[i] = given[i] + extra
            surplus = surplus - extra
    return np.array([reach] + given)


def uneven_parts(rng, number_of, total, most, lean):
    if number_of == 2:
        one = jax.random.randint(rng, (), max(1, total - most), min(most, total - 1) + 1)
        return jnp.stack([one, total - one])
    sizes = jnp.asarray(length_profile(number_of, total, most, lean), jnp.int32)
    twos = (number_of - 1) // 2
    source_of, sink = sizes[1:1 + 2 * twos:2], sizes[2:2 + 2 * twos:2]
    slack = jnp.minimum(source_of - 1, most - sink)
    passed = jax.random.randint(jax.random.fold_in(rng, 1), (twos,), 0, 1 << 20) % (slack + 1)
    sizes = sizes.at[1:1 + 2 * twos:2].set(source_of - passed).at[2:2 + 2 * twos:2].set(sink + passed)
    return sizes[jax.random.permutation(jax.random.fold_in(rng, 2), number_of)]


def scatter_about(rng, extent, spread, limit, cuts=(), held_as=jnp.bfloat16):
    result = jax.random.normal(rng, extent, jnp.float32) * spread
    if len(cuts) > 0:
        result = level_of(rng, extent, cuts, -0.22, 0.18) * result
    return jnp.clip(result, min=-limit, max=limit).astype(held_as)


def setup_inputs(seed: int = 0) -> dict:
    splits = jax.random.split(jax.random.key(seed), 9)
    return {
        "tokens": scatter_about(splits[0], (TOKENS, D), 1.0, 6.0, ((0, 8), (1, 4))),
        "out_grad": scatter_about(splits[1], (TOKENS, D), (16 * N_ROW), 768.0, ((0, 8), (1, 4))),
        "counts": draw_counts(jax.random.fold_in(splits[8], 71), 0),
        "block_moves": draw_block_moves(jax.random.fold_in(splits[8], 71), 0),
        "segment_ids": jnp.searchsorted(jnp.cumsum(uneven_parts(splits[4], TOKENS // 32, TOKENS, 128, 2)), jnp.arange(TOKENS), side="right").astype(jnp.int32),
        "gate_weight": scatter_about(splits[5], (D, F), D ** -0.5, 0.125, ((0, 8), (1, 4))),
        "up_weight": scatter_about(splits[6], (D, F), D ** -0.5, 0.125, ((0, 8), (1, 4))),
        "down_weight": scatter_about(splits[7], (D, F), F ** -0.5, 0.0625, ((0, 8), (1, 4))),
    }


def loss_mask(counts, segment_ids):
    segments = segment_ids.reshape(N_ROW, TOK_DEV)
    following = jnp.concatenate([segments[:, 1:], segments[:, -1:]], axis=1)
    places = jnp.arange(TOK_DEV, dtype=jnp.int32)[None, :]
    kept_flag = (places + 1 < counts[:, None]) & (following == segments)
    return kept_flag.astype(jnp.float32)


def work_index(counts, block_moves):
    source = block_moves[:, 0]
    target = block_moves[:, 1]
    block_id = block_moves[:, 2]
    rank_ids = jnp.arange(N_ROW, dtype=jnp.int32)
    block_ids = jnp.arange(CAP, dtype=jnp.int32)
    filled = (counts + BLOCK - 1) // BLOCK
    moved_out = jnp.any((source[None, None, :] == rank_ids[:, None, None]) & (block_id[None, None, :] == block_ids[None, :, None]), axis=2)
    kept_flag = (block_ids[None, :] < filled[:, None]) & jnp.logical_not(moved_out)
    arrive = target[None, :] == rank_ids[:, None]
    flag_bits = jnp.concatenate([kept_flag, arrive], axis=1).astype(jnp.int32)
    own_ids = (rank_ids[:, None] * CAP + block_ids[None, :]).astype(jnp.int32)
    came_ids = jnp.broadcast_to((source * CAP + block_id)[None, :], (N_ROW, MOVES)).astype(jnp.int32)
    source_ids = jnp.concatenate([own_ids, came_ids], axis=1)
    list_place = (jnp.cumsum(flag_bits, axis=1) - 1).astype(jnp.int32)
    slot_ids = jnp.arange(WORK, dtype=jnp.int32)
    slot_hit = (flag_bits[:, :, None] == 1) & (list_place[:, :, None] == slot_ids[None, None, :])
    chosen = jnp.sum(jnp.where(slot_hit, source_ids[:, :, None] + 1, 0), axis=1).astype(jnp.int32)
    return (chosen - 1).astype(jnp.int32)


def pick_blocks(block_rows, slot_index):
    flat_index = slot_index.reshape(-1)
    picked = jnp.take(block_rows, jnp.maximum(flat_index, 0), axis=0)
    live_rows = (flat_index >= 0).reshape((-1,) + (1,) * (picked.ndim - 1))
    return jnp.where(live_rows, picked, jnp.zeros_like(picked))


def local_terms(gate_sum, up_sum, back_sum):
    logistic = jax.nn.sigmoid(gate_sum)
    activated = gate_sum * logistic
    hidden = (activated * up_sum).astype(jnp.bfloat16)
    gate_back = (back_sum * up_sum * logistic * (1.0 + gate_sum * (1.0 - logistic))).astype(jnp.bfloat16)
    up_back = (back_sum * activated).astype(jnp.bfloat16)
    return hidden, gate_back, up_back


def contract(left_side, right_side):
    return lax.dot_general(left_side, right_side, (((0,), (0,)), ((), ())), preferred_element_type=jnp.float32)


def reference(tokens, out_grad, counts, block_moves, segment_ids, gate_weight, up_weight, down_weight):
    weight_mask = loss_mask(counts, segment_ids)
    loss_total = jnp.sum(weight_mask)
    slot_index = work_index(counts, block_moves)
    work_tokens = pick_blocks(tokens.reshape(N_ROW * CAP, BLOCK, D), slot_index).reshape(N_ROW, WORK * BLOCK, D)
    work_grad = pick_blocks(out_grad.reshape(N_ROW * CAP, BLOCK, D), slot_index).reshape(N_ROW, WORK * BLOCK, D)
    work_weight = pick_blocks(weight_mask.reshape(N_ROW * CAP, BLOCK), slot_index).reshape(N_ROW, WORK * BLOCK)

    def per_rank(running, inputs):
        tok_rows, grad_rows, row_weight = inputs
        gate_sum = jnp.dot(tok_rows, gate_weight, preferred_element_type=jnp.float32)
        up_sum = jnp.dot(tok_rows, up_weight, preferred_element_type=jnp.float32)
        back_sum = jnp.dot(grad_rows, down_weight, preferred_element_type=jnp.float32) * row_weight[:, None]
        hidden, gate_back, up_back = local_terms(gate_sum, up_sum, back_sum)
        weighted = grad_rows * row_weight.astype(jnp.bfloat16)[:, None]
        new_terms = (contract(tok_rows, gate_back), contract(tok_rows, up_back), contract(weighted, hidden))
        rounded = tuple(lax.optimization_barrier((term_sum / loss_total).astype(jnp.bfloat16)).astype(jnp.float32) for term_sum in new_terms)
        return tuple(total_part + new_part for total_part, new_part in zip(running, rounded)), hidden

    zero_sums = jnp.zeros((D, F), jnp.float32)
    grad_sums, hidden_all = lax.scan(per_rank, (zero_sums, zero_sums, zero_sums), (work_tokens, work_grad, work_weight))
    return hidden_all.reshape(N_ROW * WORK * BLOCK, F), grad_sums[0], grad_sums[1], grad_sums[2]
```

```python
import jax
import jax.numpy as jnp
from jax import lax
from jax.sharding import PartitionSpec as P

BLOCK = 128
WORK = 4


def local_terms(gate_sum, up_sum, back_sum):
    logistic = jax.nn.sigmoid(gate_sum)
    activated = gate_sum * logistic
    hidden = (activated * up_sum).astype(jnp.bfloat16)
    gate_back = (back_sum * up_sum * logistic * (1.0 + gate_sum * (1.0 - logistic))).astype(
        jnp.bfloat16
    )
    up_back = (back_sum * activated).astype(jnp.bfloat16)
    return (hidden, gate_back, up_back)


def contract(left_side, right_side):
    return lax.dot_general(
        left_side, right_side, (((0,), (0,)), ((), ())), preferred_element_type=jnp.float32
    )


def ring_gather(piece):
    ranks = lax.axis_size("col")
    me = lax.axis_index("col")
    rows, cols = piece.shape
    shift = [(i, (i + 1) % ranks) for i in range(ranks)]
    whole = jnp.zeros((rows, ranks * cols), piece.dtype)
    whole = lax.dynamic_update_slice(whole, piece, (0, me * cols))
    for step in range(1, ranks):
        piece = lax.ppermute(piece, "col", shift)
        owner = (me - step + ranks) % ranks
        whole = lax.dynamic_update_slice(whole, piece, (0, owner * cols))
    return whole


STAGES = 3
CORE, FIRST, SECOND = 1, 2, 4
BOTH = FIRST | SECOND
LEAVES = ((FIRST, 0), (BOTH, 0), (SECOND, 1), (BOTH, 1))
STAYS = ((0, 0), (SECOND, 0), (0, 1), (FIRST, 1))
EVEN = LEAVES + STAYS
ORDER = EVEN + tuple((offset | CORE, half) for offset, half in EVEN)


def swap(value, offset):
    ranks = lax.axis_size("row")
    return lax.ppermute(value, "row", [(i, i ^ offset) for i in range(ranks)])


def cube_gather(shard):
    half = shard.shape[0] // 2
    blocks = {(0, 0): shard[:half], (0, 1): shard[half:]}
    first = swap(shard, FIRST)
    second = swap(shard, SECOND)
    for offset, whole in ((FIRST, first), (SECOND, second)):
        blocks[offset, 0], blocks[offset, 1] = whole[:half], whole[half:]
    blocks[BOTH, 0] = swap(blocks[FIRST, 0], SECOND)
    blocks[BOTH, 1] = swap(blocks[SECOND, 1], FIRST)
    for offset, whole in ((0, shard), (FIRST, first), (SECOND, second)):
        other = swap(whole, CORE)
        blocks[offset | CORE, 0], blocks[offset | CORE, 1] = other[:half], other[half:]
    for part in (0, 1):
        blocks[BOTH | CORE, part] = swap(blocks[BOTH, part], CORE)
    return jnp.concatenate([blocks[key] for key in ORDER], axis=0)


def relative_order(features, me_rank, ranks):
    rows, width = features.shape
    half = width // (2 * ranks)
    pieces = [
        lax.dynamic_slice(features, (0, ((me_rank ^ offset) * 2 + part) * half), (rows, half))
        for offset, part in ORDER
    ]
    return jnp.concatenate(pieces, axis=1)


def cube_scatter(left_side, right_side, term_rows):
    width = left_side.shape[1]
    unit = width // 4
    quarter = unit // 2
    near = term_rows(left_side[:, 2 * unit :], right_side).astype(jnp.bfloat16)
    leave_in = swap(near[:unit], CORE)
    stay_in = swap(near[unit:], CORE)
    leaving = (
        term_rows(left_side[:, :unit], right_side) + leave_in.astype(jnp.float32)
    ).astype(jnp.bfloat16)
    first_in = swap(leaving[:quarter], FIRST)
    second_in = swap(leaving[quarter:], SECOND)
    staying = term_rows(left_side[:, unit : 2 * unit], right_side) + stay_in.astype(jnp.float32)
    first_sum = staying[:quarter] + first_in.astype(jnp.float32)
    second_sum = staying[quarter:] + second_in.astype(jnp.float32)
    eighth = quarter // 2
    second_last = swap(first_sum[eighth:].astype(jnp.bfloat16), SECOND)
    first_last = swap(second_sum[eighth:].astype(jnp.bfloat16), FIRST)
    return jnp.concatenate(
        [
            first_sum[:eighth] + second_last.astype(jnp.float32),
            second_sum[:eighth] + first_last.astype(jnp.float32),
        ],
        axis=0,
    )


def on_device(
    tokens, out_grad, counts, block_moves, segment_ids, gate_weight, up_weight, down_weight
):
    ranks_all = lax.axis_size("row")
    me_rank = lax.axis_index("row")
    slot_rows = tokens.shape[0]
    cap_blocks = slot_rows // BLOCK
    feat_cols = tokens.shape[1]
    my_count = counts[0]
    places = jnp.arange(slot_rows, dtype=jnp.int32)
    following = jnp.concatenate([segment_ids[1:], segment_ids[-1:]])
    own_weight = ((places + 1 < my_count) & (following == segment_ids)).astype(jnp.float32)
    source = block_moves[:, 0]
    target = block_moves[:, 1]
    block_id = block_moves[:, 2]
    block_ids = jnp.arange(cap_blocks, dtype=jnp.int32)
    filled = (my_count + BLOCK - 1) // BLOCK
    moved_out = jnp.any(
        (source[None, :] == me_rank) & (block_id[None, :] == block_ids[:, None]), axis=1
    )
    kept_flag = (block_ids < filled) & jnp.logical_not(moved_out)
    arrive = target == me_rank
    flag_bits = jnp.concatenate([kept_flag, arrive]).astype(jnp.int32)
    local_ids = jnp.concatenate([block_ids, cap_blocks + source])
    list_place = jnp.cumsum(flag_bits) - 1
    slot_ids = jnp.arange(WORK, dtype=jnp.int32)
    slot_hit = (flag_bits[:, None] == 1) & (list_place[:, None] == slot_ids[None, :])
    slot_index = jnp.sum(jnp.where(slot_hit, local_ids[:, None] + 1, 0), axis=0) - 1
    peer_ids = jnp.arange(ranks_all, dtype=jnp.int32)
    outgoing = (source[None, :] == me_rank) & (target[None, :] == peer_ids[:, None])
    send_block = jnp.sum(jnp.where(outgoing, block_id[None, :], 0), axis=1)
    send_live = jnp.any(outgoing, axis=1)
    own_both = jnp.concatenate([tokens, out_grad], axis=1).reshape(cap_blocks, BLOCK, 2 * feat_cols)
    own_mask = own_weight.astype(jnp.bfloat16).reshape(cap_blocks, BLOCK)

    def outbox(block_rows):
        chosen = jnp.take(block_rows, send_block, axis=0)
        live_rows = send_live.reshape((-1,) + (1,) * (chosen.ndim - 1))
        return jnp.where(live_rows, chosen, jnp.zeros_like(chosen))

    whole_count = jnp.sum(own_weight).astype(jnp.int32)
    count_parts = jnp.broadcast_to(
        jnp.stack([whole_count // 256, whole_count % 256]).astype(jnp.bfloat16)[None, :],
        (ranks_all, 2),
    )
    got_both = lax.all_to_all(outbox(own_both), "row", split_axis=0, concat_axis=0, tiled=True)
    got_small = lax.all_to_all(
        jnp.concatenate([outbox(own_mask), count_parts], axis=1),
        "row",
        split_axis=0,
        concat_axis=0,
        tiled=True,
    )
    got_mask = got_small[:, :BLOCK]
    part_values = got_small[:, BLOCK:].astype(jnp.float32)
    loss_total = 256.0 * jnp.sum(part_values[:, 0]) + jnp.sum(part_values[:, 1])

    def to_work(pool_rows):
        chosen = jnp.take(pool_rows, jnp.maximum(slot_index, 0), axis=0)
        live_rows = (slot_index >= 0).reshape((-1,) + (1,) * (chosen.ndim - 1))
        return jnp.where(live_rows, chosen, jnp.zeros_like(chosen))

    work_both = to_work(jnp.concatenate([own_both, got_both])).reshape(WORK * BLOCK, 2 * feat_cols)
    work_mask = to_work(jnp.concatenate([own_mask, got_mask])).reshape(WORK * BLOCK)
    work_weight = work_mask.astype(jnp.float32)
    hidden_cols = gate_weight.shape[1]
    cube = ranks_all == 1 << STAGES
    token_piece = work_both[:, :feat_cols]
    grad_piece = work_both[:, feat_cols:]
    if cube:
        gate_piece = cube_gather(gate_weight)
        up_later, down_later, _ = lax.optimization_barrier((up_weight, down_weight, got_both))
        up_piece = cube_gather(up_later)
        down_piece = cube_gather(down_later)
        full_tokens = relative_order(ring_gather(token_piece), me_rank, ranks_all)
        full_grad = relative_order(ring_gather(grad_piece), me_rank, ranks_all)
    else:
        full_tokens = ring_gather(token_piece)
        full_grad = ring_gather(grad_piece)
        gate_piece = lax.all_gather(gate_weight, "row", axis=0, tiled=True)
        up_piece = lax.all_gather(up_weight, "row", axis=0, tiled=True)
        down_piece = lax.all_gather(down_weight, "row", axis=0, tiled=True)
    gate_sum = jnp.dot(full_tokens, gate_piece, preferred_element_type=jnp.float32)
    up_sum = jnp.dot(full_tokens, up_piece, preferred_element_type=jnp.float32)
    back_raw = jnp.dot(full_grad, down_piece, preferred_element_type=jnp.float32)
    back_sum = back_raw * work_weight[:, None]
    hidden, gate_back, up_back = local_terms(gate_sum, up_sum, back_sum)
    weighted = full_grad * work_mask[:, None]

    def term_rows(left_side, right_side):
        return contract(left_side, right_side) / loss_total

    if cube:
        down_grad = cube_scatter(weighted, hidden, term_rows)
        gate_grad = cube_scatter(full_tokens, gate_back, term_rows)
        up_grad = cube_scatter(full_tokens, up_back, term_rows)
        return (hidden, gate_grad, up_grad, down_grad)

    down_grad = lax.psum_scatter(
        term_rows(weighted, hidden).astype(jnp.bfloat16), "row", scatter_dimension=0, tiled=True
    ).astype(jnp.float32)
    other_part = lax.psum_scatter(
        jnp.concatenate(
            [term_rows(full_tokens, gate_back), term_rows(full_tokens, up_back)], axis=1
        ).astype(jnp.bfloat16),
        "row",
        scatter_dimension=0,
        tiled=True,
    ).astype(jnp.float32)
    gate_grad = other_part[:, :hidden_cols]
    up_grad = other_part[:, hidden_cols:]
    return (hidden, gate_grad, up_grad, down_grad)


def solution(mesh):
    placed = (
        P("row", "col"),
        P("row", "col"),
        P("row"),
        P(),
        P("row"),
        P("row", "col"),
        P("row", "col"),
        P("row", "col"),
    )
    return jax.shard_map(
        on_device,
        mesh=mesh,
        in_specs=placed,
        out_specs=(P("row", "col"), P("row", "col"), P("row", "col"), P("row", "col")),
        check_vma=False,
    )
```
